32 devices in a mesh: row: 4 (over x, core), col: 8 (over z, y).
Axes of the slice: x: 2, y: 2, z: 4, core: 2. Of those that a mesh axis runs over, the one named last changes fastest.
Arguments:
- inputs: bfloat16 [512, 8192], P('col', 'row'), may hold values from -6 to 6
- cotangent: bfloat16 [512, 8192], P('col', 'row'), may hold values from -6 to 6
- gate_pre: bfloat16 [512, 16384], P('row', 'col'), may hold values from -8 to 8
- up_pre: bfloat16 [512, 16384], P('row', 'col'), may hold values from -6 to 6
- w_gate: bfloat16 [8192, 16384], P('row', 'col'), may hold values from -0.0625 to 0.0625
- w_up: bfloat16 [8192, 16384], P('row', 'col'), may hold values from -0.0625 to 0.0625
- w_down: bfloat16 [16384, 8192], P('col', 'row'), may hold values from -0.046875 to 0.046875
Outputs:
- grad_inputs: bfloat16 [512, 8192], P('col', 'row')
- grad_gate: float32 [8192, 16384], P('row', 'col')
- grad_up: float32 [8192, 16384], P('row', 'col')
- grad_down: float32 [16384, 8192], P('col', 'row')
The draws below stay inside these ranges and needn't reach their ends.
All inputs are finite; a program needn't handle non-finite values.
Results may differ from the reference program's by a relative error of at most 0.0049.
Values may be sent and summed in bfloat16 or wider, within the bound.
A program may use at most 128 MiB of HBM per device.

```python
import math
import jax
import jax.numpy as jnp

D = 8192
FF = 16384
TOKENS = 512


def block_scale(own_key, extent, shards, smallest, largest):
    gain = 1.0
    for axis_at, parts in shards:
        draws = jax.random.uniform(jax.random.fold_in(jax.random.fold_in(own_key, 6), axis_at), (parts,), jnp.float32, smallest / len(shards), largest / len(shards))
        gain = gain * jnp.repeat(jnp.exp(draws), extent[axis_at] // parts).reshape((-1,) + (1,) * (len(extent) - 1 - axis_at))
    return gain


def normal_values(own_key, dims, spread, most, cuts=(), kind=jnp.bfloat16):
    level = block_scale(own_key, dims, cuts, -0.22, 0.18) if cuts else 1.0
    entries = jax.random.normal(own_key, dims, jnp.float32) * spread * level
    return jnp.minimum(jnp.maximum(entries, -most), most).astype(kind)


def setup_inputs(seed: int = 0) -> dict:
    splits = jax.random.split(jax.random.key(seed), 8)
    return {
        "inputs": normal_values(splits[0], (TOKENS, D), 1.0, 6.0, ((0, 8), (1, 4))),
        "cotangent": normal_values(splits[1], (TOKENS, D), 1.0, 6.0, ((0, 8), (1, 4))),
        "gate_pre": normal_values(splits[2], (TOKENS, FF), 1.5, 8.0, ((0, 4), (1, 8))),
        "up_pre": normal_values(splits[3], (TOKENS, FF), 1.0, 6.0, ((0, 4), (1, 8))),
        "w_gate": normal_values(splits[4], (D, FF), D ** -0.5, 0.0625, ((0, 4), (1, 8))),
        "w_up": normal_values(splits[5], (D, FF), D ** -0.5, 0.0625, ((0, 4), (1, 8))),
        "w_down": normal_values(splits[6], (FF, D), FF ** -0.5, 0.046875, ((0, 8), (1, 4))),
    }


def reference(inputs, cotangent, gate_pre, up_pre, w_gate, w_up, w_down):
    gate_f = gate_pre.astype(jnp.float32)
    up_f = up_pre.astype(jnp.float32)
    sig = jax.nn.sigmoid(gate_f)
    act = gate_f * sig
    hidden = (act * up_f).astype(jnp.bfloat16)
    grad_hidden = jnp.dot(cotangent, w_down.T, preferred_element_type=jnp.float32)
    grad_gate_pre = (grad_hidden * up_f * sig * (1.0 + gate_f * (1.0 - sig))).astype(jnp.bfloat16)
    grad_up_pre = (grad_hidden * act).astype(jnp.bfloat16)
    grad_inputs = jnp.dot(grad_gate_pre, w_gate.T, preferred_element_type=jnp.float32)
    grad_inputs = grad_inputs + jnp.dot(grad_up_pre, w_up.T, preferred_element_type=jnp.float32)
    scale = 1.0 / math.sqrt(inputs.shape[0])
    grad_gate = jnp.dot(inputs.T, grad_gate_pre, preferred_element_type=jnp.float32) * scale
    grad_up = jnp.dot(inputs.T, grad_up_pre, preferred_element_type=jnp.float32) * scale
    grad_down = jnp.dot(hidden.T, cotangent, preferred_element_type=jnp.float32) * scale
    return (grad_inputs.astype(jnp.bfloat16), grad_gate, grad_up, grad_down)
```

```python
import math

import jax
import jax.numpy as jnp
from jax import lax
from jax.experimental import pallas as pl
from jax.experimental.pallas import tpu as pltpu
from jax.sharding import PartitionSpec as P


F32 = jnp.float32
BF16 = jnp.bfloat16
GRANT = 60 * 1024 * 1024


def tile_of(extent, most):
    tile = min(extent, most)
    while extent % tile:
        tile //= 2
    return tile


def resident(shape):
    return pl.BlockSpec(shape, lambda i: (0,) * len(shape))


def call(body, operands, in_specs, outs, out_specs, scratch, steps, flops):
    moved = sum(a.size * a.dtype.itemsize for a in list(operands) + list(outs))
    return pl.pallas_call(
        body,
        grid=(steps,),
        in_specs=in_specs,
        out_specs=out_specs,
        scratch_shapes=scratch,
        out_shape=outs,
        compiler_params=pltpu.CompilerParams(
            dimension_semantics=("arbitrary",), vmem_limit_bytes=GRANT
        ),
        cost_estimate=pl.CostEstimate(flops=flops, bytes_accessed=moved, transcendentals=0),
    )(*operands)


def dot_nt(left, right):
    return lax.dot_general(left, right, (((1,), (1,)), ((), ())), preferred_element_type=F32)


def where(rows, cols):
    groups, lines = rows // 2, cols // 2
    r, c = lax.axis_index("row"), lax.axis_index("col")
    g, core, z, y = lax.div(r, 2), lax.rem(r, 2), lax.div(c, 2), lax.rem(c, 2)
    back = [lax.rem(z - k + lines, lines) for k in range(lines)]
    ahead = [lax.rem(z + k, lines) for k in range(lines)]
    ring = [lax.rem(g + j, groups) for j in range(groups)]
    col_at = [2 * v + y for v in back] + [2 * v + 1 - y for v in back]
    row_at = [2 * v + core for v in ring] + [2 * v + 1 - core for v in ring]
    pick = [2 * v + 1 - y for v in ahead] + [2 * v + y for v in ahead]
    return col_at, row_at, pick


def hidden_grad(mesh, blocks, w_down, part, parts):
    rows, cols = mesh
    count, depth, wide = len(blocks), blocks[0].shape[-1], w_down.shape[0] // parts
    chunk, fresh = blocks[0].shape[0], count > 1
    tokens, tile = count * chunk, tile_of(wide, 256)
    per, half, steps = tokens // rows, rows // 2, wide // tile

    def body(*refs):
        ins, w, mine, theirs, total = refs[:count], refs[count], *refs[count + 1:count + 3], refs[-1]
        col_at, row_at, _ = where(rows, cols)
        if fresh:
            held = refs[count + 3]

            @pl.when(pl.program_id(0) == 0)
            def _():
                for at, ref in zip(col_at, ins):
                    held[at] = ref[...]

            left = held[...].reshape(tokens, depth)
        else:
            left = ins[0][...]
        total[...] = dot_nt(left, w[...]).reshape(rows, per, tile)
        for j in range(half):
            mine[j] = total[row_at[j]]
            theirs[j] = total[row_at[half + j]]

    outs = [jax.ShapeDtypeStruct((half, per, wide), F32)] * 2
    out_specs = [pl.BlockSpec((half, per, tile), lambda i: (0, 0, i))] * 2
    if fresh:
        outs.append(jax.ShapeDtypeStruct((count, chunk, depth), BF16))
        out_specs.append(resident((count, chunk, depth)))
    got = call(
        body, (*blocks, w_down),
        [resident((chunk, depth))] * count
        + [pl.BlockSpec((tile, depth), lambda i: (i + part * steps, 0))],
        outs, out_specs, [pltpu.VMEM((rows, per, tile), F32)], steps, 2 * tokens * depth * wide,
    )
    return got[0], got[1], (got[2].reshape(tokens, depth) if fresh else blocks[0])


def input_grad(mesh, gates, ups, w_gate, w_up, part, parts):
    rows, cols = mesh
    fresh = len(gates) > 1
    count, depth, wide = len(gates), w_gate.shape[1], w_gate.shape[0] // parts
    tokens = rows * gates[0].shape[1] if fresh else gates[0].shape[0]
    tile, half, lines = tile_of(wide, 256), rows // 2, cols // 2
    per, steps, block = tokens // cols, wide // tile, tokens // rows

    def body(*refs):
        wg, wu, send, keep = refs[2 * count:2 * count + 4]
        _, row_at, pick = where(rows, cols)
        if fresh:
            wholes = refs[2 * count + 4:2 * count + 6]

            @pl.when(pl.program_id(0) == 0)
            def _():
                for whole, ins in zip(wholes, (refs[:count], refs[count:2 * count])):
                    for n, ref in enumerate(ins):
                        width = ref.shape[-1]
                        at = n // 2 * width
                        for j in range(half):
                            whole[row_at[n % 2 * half + j], :, at:at + width] = ref[j]

            left = [w[...].reshape(tokens, depth) for w in wholes]
        else:
            left = [refs[0][...], refs[1][...]]
        total = refs[-1]
        total[...] = (dot_nt(left[0], wg[...]) + dot_nt(left[1], wu[...])).reshape(cols, per, tile)
        for k in range(lines):
            send[k] = total[pick[k]].astype(BF16)
            keep[k] = total[pick[lines + k]]

    weight = pl.BlockSpec((tile, depth), lambda i: (i + part * steps, 0))
    outs = [jax.ShapeDtypeStruct((lines, per, wide), t) for t in (BF16, F32)]
    out_specs = [pl.BlockSpec((lines, per, tile), lambda i: (0, 0, i))] * 2
    if fresh:
        outs += [jax.ShapeDtypeStruct((rows, block, depth), BF16)] * 2
        out_specs += [resident((rows, block, depth))] * 2
    got = call(
        body, (*gates, *ups, w_gate, w_up),
        [resident(a.shape) for a in (*gates, *ups)] + [weight] * 2,
        outs, out_specs, [pltpu.VMEM((cols, per, tile), F32)], steps, 4 * tokens * depth * wide,
    )
    if not fresh:
        return got[0], got[1], gates[0], ups[0]
    return got[0], got[1], got[2].reshape(tokens, depth), got[3].reshape(tokens, depth)


def outer(mesh, left, by_row, right, scale):
    rows, cols = mesh
    tokens, wide = right.shape
    count, spread = len(left), left[0].shape[-1]
    tile, size = tile_of(spread, 256), left[0].shape[1]
    every = sum(a.shape[0] for a in left)

    def body(*refs):
        right_ref, out, held = refs[count:]
        at = where(rows, cols)[1 if by_row else 0]
        n = 0
        for ref in refs[:count]:
            for j in range(ref.shape[0]):
                held[at[n]] = ref[j]
                n += 1
        out[...] = lax.dot_general(
            held[...].reshape(tokens, tile), right_ref[...],
            (((0,), (0,)), ((), ())), preferred_element_type=F32,
        ) * scale

    return call(
        body, (*left, right),
        [pl.BlockSpec((a.shape[0], size, tile), lambda i: (0, 0, i)) for a in left]
        + [resident((tokens, wide))],
        [jax.ShapeDtypeStruct((spread, wide), F32)],
        [pl.BlockSpec((tile, wide), lambda i: (i, 0))],
        [pltpu.VMEM((every, size, tile), BF16)], spread // tile, 2 * tokens * spread * wide,
    )[0]


PARTS = 2


def per_device(mesh, inputs, cotangent, gate_pre, up_pre, w_gate, w_up, w_down):
    rows, cols = mesh
    groups, lines = rows // 2, cols // 2

    def twin(x, axis, size):
        return lax.ppermute(x, axis, [(i, i ^ 1) for i in range(size)])

    def shift(x, axis, size, k):
        return lax.ppermute(x, axis, [(i, (i + 2 * k) % size) for i in range(size)])

    gates = [gate_pre] + [shift(gate_pre, "row", rows, -j) for j in range(1, groups)]
    ups = [up_pre] + [shift(up_pre, "row", rows, -j) for j in range(1, groups)]
    cot = [cotangent] + [shift(cotangent, "col", cols, k) for k in range(1, lines)]
    gate_f, up_f = jnp.stack(gates).astype(F32), jnp.stack(ups).astype(F32)
    sig = jax.nn.sigmoid(gate_f)
    act = gate_f * sig
    hid = (act * up_f).astype(BF16)
    slope = up_f * sig * (1.0 + gate_f * (1.0 - sig))
    cot[1], hid, slope, act = lax.optimization_barrier((cot[1], hid, slope, act))
    cot += [twin(b, "col", cols) for b in cot]
    hid = [hid, twin(hid, "row", rows)]

    blocks, sums, moving = cot, [], []
    for h in range(PARTS):
        mine, theirs, cot_all = hidden_grad(mesh, blocks, w_down, h, PARTS)
        blocks = [cot_all]
        if h == 0:
            mine, theirs, x_late = lax.optimization_barrier((mine, theirs, inputs))
            xs = [x_late] + [shift(x_late, "col", cols, k) for k in range(1, lines)]
        mine = mine + twin(theirs, "row", rows)
        sent = mine.astype(BF16)
        moving.append([shift(sent, "row", rows, k) for k in range(1, groups)])
        sums.append(mine)
    scale = 1.0 / math.sqrt(cot_all.shape[0])
    grad_down = outer(mesh, hid, True, cot_all, scale)
    xs += [twin(b, "col", cols) for b in xs]
    xs = [b[None] for b in xs]

    gate_grads, up_grads = [], []
    width = gate_pre.shape[1] // PARTS
    for h in range(PARTS):
        total = sums[h]
        for k, got in enumerate(moving[h], 1):
            got = got.astype(F32)
            total = total + jnp.stack([got[(j + k) % groups] for j in range(groups)])
        at = slice(h * width, (h + 1) * width)
        gate_grad = (total * slope[:, :, at]).astype(BF16)
        up_grad = (total * act[:, :, at]).astype(BF16)
        gate_grads += [gate_grad, twin(gate_grad, "row", rows)]
        up_grads += [up_grad, twin(up_grad, "row", rows)]

    results = []
    for h in range(PARTS):
        send, keep, gate_all, up_all = input_grad(
            mesh, gate_grads, up_grads, w_gate, w_up, h, PARTS
        )
        gate_grads, up_grads = [gate_all], [up_all]
        keep = keep + twin(send, "col", cols).astype(F32)
        out = keep[0]
        for k in range(1, lines):
            out = out + shift(keep[k].astype(BF16), "col", cols, k).astype(F32)
        results.append(out.astype(BF16))
    grad_gate = outer(mesh, xs, False, gate_all, scale)
    grad_up = outer(mesh, xs, False, up_all, scale)
    return (jnp.concatenate(results, axis=1), grad_gate, grad_up, grad_down)


def solution(mesh):
    sizes = (mesh.shape["row"], mesh.shape["col"])
    in_specs = (
        P("col", "row"),
        P("col", "row"),
        P("row", "col"),
        P("row", "col"),
        P("row", "col"),
        P("row", "col"),
        P("col", "row"),
    )
    out_specs = (P("col", "row"), P("row", "col"), P("row", "col"), P("col", "row"))

    def body(*args):
        return per_device(sizes, *args)

    return jax.shard_map(body, mesh=mesh, in_specs=in_specs, out_specs=out_specs, check_vma=False)
```

```python
import math

import jax
import jax.numpy as jnp
from jax import lax
from jax.experimental import pallas as pl
from jax.experimental.pallas import tpu as pltpu
from jax.sharding import PartitionSpec as P


F32 = jnp.float32
BF16 = jnp.bfloat16
GRANT = 60 * 1024 * 1024


def tile_of(extent, most):
    tile = min(extent, most)
    while extent % tile:
        tile //= 2
    return tile


def resident(shape):
    return pl.BlockSpec(shape, lambda i: (0,) * len(shape))


def call(body, operands, in_specs, outs, out_specs, scratch, steps, flops):
    moved = sum(a.size * a.dtype.itemsize for a in list(operands) + list(outs))
    return pl.pallas_call(
        body,
        grid=(steps,),
        in_specs=in_specs,
        out_specs=out_specs,
        scratch_shapes=scratch,
        out_shape=outs,
        compiler_params=pltpu.CompilerParams(
            dimension_semantics=("arbitrary",), vmem_limit_bytes=GRANT
        ),
        cost_estimate=pl.CostEstimate(flops=flops, bytes_accessed=moved, transcendentals=0),
    )(*operands)


def dot_nt(left, right):
    return lax.dot_general(left, right, (((1,), (1,)), ((), ())), preferred_element_type=F32)


def where(rows, cols):
    groups, lines = rows // 2, cols // 2
    r, c = lax.axis_index("row"), lax.axis_index("col")
    g, core, z, y = lax.div(r, 2), lax.rem(r, 2), lax.div(c, 2), lax.rem(c, 2)
    back = [lax.rem(z - k + lines, lines) for k in range(lines)]
    ahead = [lax.rem(z + k, lines) for k in range(lines)]
    ring = [lax.rem(g + j, groups) for j in range(groups)]
    col_at = [2 * v + y for v in back] + [2 * v + 1 - y for v in back]
    row_at = [2 * v + core for v in ring] + [2 * v + 1 - core for v in ring]
    pick = [2 * v + 1 - y for v in ahead] + [2 * v + y for v in ahead]
    return col_at, row_at, pick


def hidden_grad(mesh, blocks, w_down, part, parts):
    rows, cols = mesh
    count, depth, wide = len(blocks), blocks[0].shape[-1], w_down.shape[0] // parts
    chunk, fresh = blocks[0].shape[0], count > 1
    tokens, tile = count * chunk, tile_of(wide, 256)
    per, half, steps = tokens // rows, rows // 2, wide // tile

    def body(*refs):
        ins, w, mine, theirs, total = refs[:count], refs[count], *refs[count + 1:count + 3], refs[-1]
        col_at, row_at, _ = where(rows, cols)
        if fresh:
            held = refs[count + 3]

            @pl.when(pl.program_id(0) == 0)
            def _():
                for at, ref in zip(col_at, ins):
                    held[at] = ref[...]

            left = held[...].reshape(tokens, depth)
        else:
            left = ins[0][...]
        total[...] = dot_nt(left, w[...]).reshape(rows, per, tile)
        for j in range(half):
            mine[j] = total[row_at[j]]
            theirs[j] = total[row_at[half + j]]

    outs = [jax.ShapeDtypeStruct((half, per, wide), F32)] * 2
    out_specs = [pl.BlockSpec((half, per, tile), lambda i: (0, 0, i))] * 2
    if fresh:
        outs.append(jax.ShapeDtypeStruct((count, chunk, depth), BF16))
        out_specs.append(resident((count, chunk, depth)))
    got = call(
        body, (*blocks, w_down),
        [resident((chunk, depth))] * count
        + [pl.BlockSpec((tile, depth), lambda i: (i + part * steps, 0))],
        outs, out_specs, [pltpu.VMEM((rows, per, tile), F32)], steps, 2 * tokens * depth * wide,
    )
    return got[0], got[1], (got[2].reshape(tokens, depth) if fresh else blocks[0])


def input_grad(mesh, gates, ups, w_gate, w_up, part, parts):
    rows, cols = mesh
    fresh = len(gates) > 1
    count, depth, wide = len(gates), w_gate.shape[1], w_gate.shape[0] // parts
    tokens = rows * gates[0].shape[1] if fresh else gates[0].shape[0]
    tile, half, lines = tile_of(wide, 256), rows // 2, cols // 2
    per, steps, block = tokens // cols, wide // tile, tokens // rows

    def body(*refs):
        wg, wu, send, keep = refs[2 * count:2 * count + 4]
        _, row_at, pick = where(rows, cols)
        if fresh:
            wholes = refs[2 * count + 4:2 * count + 6]

            @pl.when(pl.program_id(0) == 0)
            def _():
                for whole, ins in zip(wholes, (refs[:count], refs[count:2 * count])):
                    for n, ref in enumerate(ins):
                        width = ref.shape[-1]
                        at = n // 2 * width
                        for j in range(half):
                            whole[row_at[n % 2 * half + j], :, at:at + width] = ref[j]

            left = [w[...].reshape(tokens, depth) for w in wholes]
        else:
            left = [refs[0][...], refs[1][...]]
        total = refs[-1]
        total[...] = (dot_nt(left[0], wg[...]) + dot_nt(left[1], wu[...])).reshape(cols, per, tile)
        for k in range(lines):
            send[k] = total[pick[k]].astype(BF16)
            keep[k] = total[pick[lines + k]]

    weight = pl.BlockSpec((tile, depth), lambda i: (i + part * steps, 0))
    outs = [jax.ShapeDtypeStruct((lines, per, wide), t) for t in (BF16, F32)]
    out_specs = [pl.BlockSpec((lines, per, tile), lambda i: (0, 0, i))] * 2
    if fresh:
        outs += [jax.ShapeDtypeStruct((rows, block, depth), BF16)] * 2
        out_specs += [resident((rows, block, depth))] * 2
    got = call(
        body, (*gates, *ups, w_gate, w_up),
        [resident(a.shape) for a in (*gates, *ups)] + [weight] * 2,
        outs, out_specs, [pltpu.VMEM((cols, per, tile), F32)], steps, 4 * tokens * depth * wide,
    )
    if not fresh:
        return got[0], got[1], gates[0], ups[0]
    return got[0], got[1], got[2].reshape(tokens, depth), got[3].reshape(tokens, depth)


def outer(mesh, left, by_row, right, scale):
    rows, cols = mesh
    tokens, wide = right.shape
    count, spread = len(left), left[0].shape[-1]
    tile, size = tile_of(spread, 512), left[0].shape[1]
    every = sum(a.shape[0] for a in left)

    def body(*refs):
        right_ref, out, held = refs[count:]
        at = where(rows, cols)[1 if by_row else 0]
        n = 0
        for ref in refs[:count]:
            for j in range(ref.shape[0]):
                held[at[n]] = ref[j]
                n += 1
        out[...] = lax.dot_general(
            held[...].reshape(tokens, tile), right_ref[...],
            (((0,), (0,)), ((), ())), preferred_element_type=F32,
        ) * scale

    return call(
        body, (*left, right),
        [pl.BlockSpec((a.shape[0], size, tile), lambda i: (0, 0, i)) for a in left]
        + [resident((tokens, wide))],
        [jax.ShapeDtypeStruct((spread, wide), F32)],
        [pl.BlockSpec((tile, wide), lambda i: (i, 0))],
        [pltpu.VMEM((every, size, tile), BF16)], spread // tile, 2 * tokens * spread * wide,
    )[0]


PARTS = 2


def per_device(mesh, inputs, cotangent, gate_pre, up_pre, w_gate, w_up, w_down):
    rows, cols = mesh
    groups, lines = rows // 2, cols // 2

    def twin(x, axis, size):
        return lax.ppermute(x, axis, [(i, i ^ 1) for i in range(size)])

    def shift(x, axis, size, k):
        return lax.ppermute(x, axis, [(i, (i + 2 * k) % size) for i in range(size)])

    gates = [gate_pre] + [shift(gate_pre, "row", rows, -j) for j in range(1, groups)]
    ups = [up_pre] + [shift(up_pre, "row", rows, -j) for j in range(1, groups)]
    cot = [cotangent] + [shift(cotangent, "col", cols, k) for k in range(1, lines)]
    gate_f, up_f = jnp.stack(gates).astype(F32), jnp.stack(ups).astype(F32)
    sig = jax.nn.sigmoid(gate_f)
    act = gate_f * sig
    hid = (act * up_f).astype(BF16)
    slope = up_f * sig * (1.0 + gate_f * (1.0 - sig))
    cot[1], hid, slope, act = lax.optimization_barrier((cot[1], hid, slope, act))
    cot += [twin(b, "col", cols) for b in cot]
    cot[-2], x_late = lax.optimization_barrier((cot[-2], inputs))
    xs = [x_late] + [shift(x_late, "col", cols, k) for k in range(1, lines)]
    hid = [hid, twin(hid, "row", rows)]

    blocks, sums, moving = cot, [], []
    for h in range(PARTS):
        mine, theirs, cot_all = hidden_grad(mesh, blocks, w_down, h, PARTS)
        blocks = [cot_all]
        mine = mine + twin(theirs, "row", rows)
        sent = mine.astype(BF16)
        moving.append([shift(sent, "row", rows, k) for k in range(1, groups)])
        sums.append(mine)
    scale = 1.0 / math.sqrt(cot_all.shape[0])
    grad_down = outer(mesh, hid, True, cot_all, scale)
    xs += [twin(b, "col", cols) for b in xs]
    xs = [b[None] for b in xs]

    gate_grads, up_grads = [], []
    width = gate_pre.shape[1] // PARTS
    for h in range(PARTS):
        total = sums[h]
        for k, got in enumerate(moving[h], 1):
            got = got.astype(F32)
            total = total + jnp.stack([got[(j + k) % groups] for j in range(groups)])
        at = slice(h * width, (h + 1) * width)
        gate_grad = (total * slope[:, :, at]).astype(BF16)
        up_grad = (total * act[:, :, at]).astype(BF16)
        gate_grads += [gate_grad, twin(gate_grad, "row", rows)]
        up_grads += [up_grad, twin(up_grad, "row", rows)]

    results = []
    for h in range(PARTS):
        send, keep, gate_all, up_all = input_grad(
            mesh, gate_grads, up_grads, w_gate, w_up, h, PARTS
        )
        gate_grads, up_grads = [gate_all], [up_all]
        keep = keep + twin(send, "col", cols).astype(F32)
        out = keep[0]
        for k in range(1, lines):
            out = out + shift(keep[k].astype(BF16), "col", cols, k).astype(F32)
        results.append(out.astype(BF16))
    grad_gate = outer(mesh, xs, False, gate_all, scale)
    grad_up = outer(mesh, xs, False, up_all, scale)
    return (jnp.concatenate(results, axis=1), grad_gate, grad_up, grad_down)


def solution(mesh):
    sizes = (mesh.shape["row"], mesh.shape["col"])
    in_specs = (
        P("col", "row"),
        P("col", "row"),
        P("row", "col"),
        P("row", "col"),
        P("row", "col"),
        P("row", "col"),
        P("col", "row"),
    )
    out_specs = (P("col", "row"), P("row", "col"), P("row", "col"), P("col", "row"))

    def body(*args):
        return per_device(sizes, *args)

    return jax.shard_map(body, mesh=mesh, in_specs=in_specs, out_specs=out_specs, check_vma=False)
```
